128 devices in a mesh: data: 1, pair: 128 (over z, y, x, core).
Axes of the slice: x: 4, y: 4, z: 4, core: 2. Of those that a mesh axis runs over, the one named last changes fastest.
Arguments:
- x_enc: bfloat16 [2048, 256, 512], P(('data', 'pair'))
- enc_len: int32 [2048], P(('data', 'pair'))
- y_dec: bfloat16 [2048, 32, 512], P(('data', 'pair'))
- enc_wq: bfloat16 [2, 512, 512], replicated
- enc_wk: bfloat16 [2, 512, 512], replicated
- enc_wv: bfloat16 [2, 512, 512], replicated
- enc_wo: bfloat16 [2, 8, 64, 512], replicated
- enc_w1: bfloat16 [2, 512, 2048], replicated
- enc_w2: bfloat16 [2, 2048, 512], replicated
- dec_wq: bfloat16 [2, 512, 512], replicated
- dec_wk: bfloat16 [2, 512, 512], replicated
- dec_wv: bfloat16 [2, 512, 512], replicated
- dec_wo: bfloat16 [2, 8, 64, 512], replicated
- crs_wq: bfloat16 [2, 512, 512], replicated
- crs_wk: bfloat16 [2, 512, 512], replicated
- crs_wv: bfloat16 [2, 512, 512], replicated
- crs_wo: bfloat16 [2, 8, 64, 512], replicated
- dec_w1: bfloat16 [2, 512, 2048], replicated
- dec_w2: bfloat16 [2, 2048, 512], replicated
Outputs:
- output: bfloat16 [2048, 32, 512], P(('data', 'pair'))
All inputs are finite; a program needn't handle non-finite values.
Results may differ from the reference program's by a relative error of at most 0.0110627.
Values are sent between devices in bfloat16 or wider.
A program may use at most 1 GiB of HBM per device.

```python
import jax
import jax.numpy as jnp
from jax import lax

BATCH_ROWS = 2048
SEQ_ENC = 256
SEQ_DEC = 32
D_MODEL = 512
NUM_HEADS = 8
KV_HEADS = 8
HEAD_DIM = 64
FF_DIM = 2048
ENC_LAYERS = 2
DEC_LAYERS = 2


def setup_inputs(seed: int = 0, part: int = 0) -> dict:
    base_key = jax.random.key(seed)
    part_key = jax.random.fold_in(base_key, part)
    x_key, y_key = jax.random.split(part_key, 2)
    len_key = jax.random.fold_in(part_key, 3)
    weight_keys = jax.random.split(jax.random.key(seed + 1), 16)
    q_width = NUM_HEADS * HEAD_DIM
    kv_width = KV_HEADS * HEAD_DIM
    in_scale = D_MODEL ** -0.5
    out_scale = q_width ** -0.5
    attn_boost = SEQ_ENC ** 0.5 / 3.0

    def draw_normal(key, shape, scale):
        return (jax.random.normal(key, shape, jnp.float32) * scale).astype(jnp.bfloat16)

    enc_len = jax.random.randint(len_key, (BATCH_ROWS,), SEQ_ENC // 4, SEQ_ENC + 1, dtype=jnp.int32)
    enc_len = enc_len.at[0].set(SEQ_ENC).at[1].set(SEQ_ENC // 4)
    return {
        "x_enc": draw_normal(x_key, (BATCH_ROWS, SEQ_ENC, D_MODEL), 1.0),
        "enc_len": enc_len,
        "y_dec": draw_normal(y_key, (BATCH_ROWS, SEQ_DEC, D_MODEL), 1.0),
        "enc_wq": draw_normal(weight_keys[0], (ENC_LAYERS, D_MODEL, q_width), in_scale),
        "enc_wk": draw_normal(weight_keys[1], (ENC_LAYERS, D_MODEL, kv_width), in_scale),
        "enc_wv": draw_normal(weight_keys[2], (ENC_LAYERS, D_MODEL, kv_width), in_scale),
        "enc_wo": draw_normal(weight_keys[3], (ENC_LAYERS, NUM_HEADS, HEAD_DIM, D_MODEL), out_scale * attn_boost),
        "enc_w1": draw_normal(weight_keys[4], (ENC_LAYERS, D_MODEL, FF_DIM), in_scale),
        "enc_w2": draw_normal(weight_keys[5], (ENC_LAYERS, FF_DIM, D_MODEL), FF_DIM ** -0.5),
        "dec_wq": draw_normal(weight_keys[6], (DEC_LAYERS, D_MODEL, q_width), in_scale),
        "dec_wk": draw_normal(weight_keys[7], (DEC_LAYERS, D_MODEL, kv_width), in_scale),
        "dec_wv": draw_normal(weight_keys[8], (DEC_LAYERS, D_MODEL, kv_width), in_scale),
        "dec_wo": draw_normal(weight_keys[9], (DEC_LAYERS, NUM_HEADS, HEAD_DIM, D_MODEL), out_scale * 1.5),
        "crs_wq": draw_normal(weight_keys[10], (DEC_LAYERS, D_MODEL, q_width), in_scale),
        "crs_wk": draw_normal(weight_keys[11], (DEC_LAYERS, D_MODEL, kv_width), in_scale),
        "crs_wv": draw_normal(weight_keys[12], (DEC_LAYERS, D_MODEL, kv_width), in_scale),
        "crs_wo": draw_normal(weight_keys[13], (DEC_LAYERS, NUM_HEADS, HEAD_DIM, D_MODEL), out_scale * attn_boost),
        "dec_w1": draw_normal(weight_keys[14], (DEC_LAYERS, D_MODEL, FF_DIM), in_scale),
        "dec_w2": draw_normal(weight_keys[15], (DEC_LAYERS, FF_DIM, D_MODEL), FF_DIM ** -0.5),
    }


def rms_norm(hidden):
    x_wide = hidden.astype(jnp.float32)
    inv_rms = lax.rsqrt(jnp.mean(x_wide * x_wide, axis=-1, keepdims=True) + 1e-6)
    return (x_wide * inv_rms).astype(jnp.bfloat16)


def project(source, weight):
    return jnp.dot(source, weight, preferred_element_type=jnp.float32).astype(jnp.bfloat16)


def add_to(hidden, update):
    return (hidden.astype(jnp.float32) + update).astype(jnp.bfloat16)


def attend(query_rows, key_rows, value_rows, allowed, out_weight):
    q_len = query_rows.shape[0]
    k_len = key_rows.shape[0]
    q_heads = query_rows.reshape(q_len, KV_HEADS, NUM_HEADS // KV_HEADS, HEAD_DIM).astype(jnp.float32)
    k_heads = key_rows.reshape(k_len, KV_HEADS, HEAD_DIM).astype(jnp.float32)
    v_heads = value_rows.reshape(k_len, KV_HEADS, HEAD_DIM).astype(jnp.float32)
    scores = jnp.einsum("skrh,tkh->krst", q_heads, k_heads) * HEAD_DIM ** -0.5
    scores = jnp.where(allowed, scores, -1e30)
    attn_probs = jax.nn.softmax(scores, axis=-1).astype(jnp.bfloat16)
    context = jnp.einsum("krst,tkh->skrh", attn_probs.astype(jnp.float32), v_heads).astype(jnp.bfloat16)
    context = context.reshape(q_len, NUM_HEADS * HEAD_DIM)
    w_out = out_weight.reshape(NUM_HEADS * HEAD_DIM, D_MODEL)
    return jnp.dot(context, w_out, preferred_element_type=jnp.float32)


def feed_forward(hidden, w_up, w_down):
    normed = rms_norm(hidden)
    inner_act = jax.nn.gelu(jnp.dot(normed, w_up, preferred_element_type=jnp.float32)).astype(jnp.bfloat16)
    return add_to(hidden, jnp.dot(inner_act, w_down, preferred_element_type=jnp.float32))


def encode_row(x_row, length, enc_weights):
    allowed = jnp.arange(SEQ_ENC)[None, :] < length

    def layer_step(hidden, layer_weights):
        w_query, w_key, w_value, w_out, w_up, w_down = layer_weights
        normed = rms_norm(hidden)
        attn_out = attend(project(normed, w_query), project(normed, w_key), project(normed, w_value), allowed, w_out)
        return feed_forward(add_to(hidden, attn_out), w_up, w_down), None

    hidden, unused = lax.scan(layer_step, x_row, enc_weights)
    return rms_norm(hidden)


def decode_row(y_row, enc_row, length, dec_weights):
    cross_ok = jnp.arange(SEQ_ENC)[None, :] < length
    causal = jnp.arange(SEQ_DEC)[:, None] >= jnp.arange(SEQ_DEC)[None, :]

    def layer_step(hidden, layer_weights):
        w_query, w_key, w_value, w_out, c_query, c_key, c_value, c_out, w_up, w_down = layer_weights
        normed = rms_norm(hidden)
        self_out = attend(project(normed, w_query), project(normed, w_key), project(normed, w_value), causal, w_out)
        hidden = add_to(hidden, self_out)
        normed = rms_norm(hidden)
        cross_out = attend(project(normed, c_query), project(enc_row, c_key), project(enc_row, c_value), cross_ok, c_out)
        return feed_forward(add_to(hidden, cross_out), w_up, w_down), None

    hidden, unused = lax.scan(layer_step, y_row, dec_weights)
    return hidden


def reference(x_enc, enc_len, y_dec, enc_wq, enc_wk, enc_wv, enc_wo, enc_w1, enc_w2, dec_wq, dec_wk, dec_wv, dec_wo, crs_wq, crs_wk, crs_wv, crs_wo, dec_w1, dec_w2):
    enc_weights = (enc_wq, enc_wk, enc_wv, enc_wo, enc_w1, enc_w2)
    dec_weights = (dec_wq, dec_wk, dec_wv, dec_wo, crs_wq, crs_wk, crs_wv, crs_wo, dec_w1, dec_w2)
    enc_out = lax.map(lambda row_in: encode_row(row_in[0], row_in[1], enc_weights), (x_enc, enc_len))
    partner_out = jnp.roll(enc_out, BATCH_ROWS // 2, axis=0)
    partner_len = jnp.roll(enc_len, BATCH_ROWS // 2, axis=0)
    return lax.map(lambda row_in: decode_row(row_in[0], row_in[1], row_in[2], dec_weights), (y_dec, partner_out, partner_len))
```

```python
import functools

import jax
import jax.numpy as jnp
from jax import lax
from jax.experimental import pallas as pl
from jax.experimental.pallas import tpu as pltpu
from jax.sharding import PartitionSpec as P

BF = jnp.bfloat16
F32 = jnp.float32
BLK = 256
GRAN = 16
HD = 64
LOG2E = 1.4426950408889634
NEG = -1e30


def dot(a, b):
    return jnp.dot(a, b, preferred_element_type=F32)


def dot_t(a, b):
    return lax.dot_general(a, b, (((1,), (1,)), ((), ())), preferred_element_type=F32)


def norm(x):
    xw = x.astype(F32)
    return (xw * lax.rsqrt(jnp.mean(xw * xw, axis=-1, keepdims=True) + 1e-6)).astype(BF)


def gelu(x):
    inner = x * (0.7978845608028654 + 0.035677408136300125 * (x * x))
    half = 0.5 * x
    return half + half * jnp.tanh(inner)


def ffn(h1, w1_ref, w2_ref, layer, u_ref):
    hn = norm(h1)
    ff = w1_ref.shape[2]
    for c in range(0, ff, 512):
        u_ref[:, c:c + 512] = gelu(dot(hn, w1_ref[layer, :, c:c + 512])).astype(BF)
    return (h1.astype(F32) + dot(u_ref[...], w2_ref[layer])).astype(BF)


def head_attention(keys, queries, vtx_ref, ctx_ref, mask=None):
    lk, lq = keys.shape[0], queries.shape[0]
    heads = keys.shape[1] // HD
    lane = lax.broadcasted_iota(jnp.int32, (lq, 2 * HD), 1)
    for h in range(heads):
        pair = slice(128 * (h // 2), 128 * (h // 2) + 128)
        mine = (lane < HD) if h % 2 == 0 else (lane >= HD)
        q = jnp.where(mine, queries[:, pair], jnp.zeros((), BF))
        s = dot_t(keys[:, pair], q)
        if mask is not None:
            s = jnp.where(mask, s, NEG)
        m = jnp.max(s, axis=0, keepdims=True)
        e = jnp.exp2((s - m) * LOG2E).astype(BF)
        o = dot(vtx_ref[h, :, :lk], e)
        ctx_ref[h * HD:(h + 1) * HD, :lq] = (o[:HD] * (1.0 / o[HD:HD + 1])).astype(BF)


def store_values(v, vtx_ref, lk):
    vt = v.T
    for h in range(v.shape[1] // HD):
        vtx_ref[h, :HD, :lk] = vt[h * HD:(h + 1) * HD]


def row_starts(len_ref, rows):
    starts = [jnp.int32(0)]
    for r in range(rows):
        starts.append(starts[-1] + (len_ref[r] + (GRAN - 1)) // GRAN * GRAN)
    return starts


def encoder_kernel(rows, seq, len_ref, x_hbm, wq_h, wk_h, wv_h, wo_h, w1_h, w2_h, cwk_h, cwv_h,
                   ck_hbm, cv_hbm,
                   h_ref, q_ref, k_ref, v_ref, c_ref, u_ref, vtx_ref, ctx_ref,
                   wq, wk, wv, wo, w1, w2, cwk, cwv, start_ref, x_sem, w_sem, o_sem):
    layers = wq.shape[0]
    x_copies = [pltpu.make_async_copy(x_hbm.at[r], q_ref.at[pl.ds(r * seq, seq)], x_sem.at[r]) for r in range(rows)]
    for copy in x_copies:
        copy.start()
    pairs = [(wq_h, wq), (wk_h, wk), (wv_h, wv), (wo_h, wo), (w1_h, w1), (w2_h, w2)]
    w_copies = {}
    for layer in range(layers):
        for i, (src, dst) in enumerate(pairs):
            w_copies[i, layer] = pltpu.make_async_copy(src.at[layer], dst.at[layer], w_sem.at[layer, i])
            w_copies[i, layer].start()
    for i, (src, dst) in enumerate([(cwk_h, cwk), (cwv_h, cwv)]):
        w_copies[6 + i, 0] = pltpu.make_async_copy(src, dst, w_sem.at[0, 6 + i])
        w_copies[6 + i, 0].start()

    starts = row_starts(len_ref, rows)
    for r in range(rows):
        start_ref[r] = starts[r]
    blocks = (starts[rows] + (BLK - 1)) // BLK
    for r in range(rows):
        x_copies[r].wait()
        h_ref[pl.ds(pl.multiple_of(starts[r], GRAN), seq)] = q_ref[pl.ds(r * seq, seq)]

    def block_at(b):
        return pl.ds(pl.multiple_of(b * BLK, BLK), BLK)

    def project(b, hidden, layer):
        hn = norm(hidden)
        at = block_at(b)
        q_ref[at] = (dot(hn, wq[layer]).astype(BF) * BF(HD ** -0.5))
        k_ref[at] = dot(hn, wk[layer]).astype(BF)
        v_ref[at] = dot(hn, wv[layer]).astype(BF)

    def attention(r, lq, lk):
        begin = pl.multiple_of(start_ref[r], GRAN)
        length = len_ref[r]
        at_k, at_q = pl.ds(begin, lk), pl.ds(begin, lq)
        inside = lax.broadcasted_iota(jnp.int32, (lk, 1), 0) < length
        keys = jnp.where(inside, k_ref[at_k], k_ref[pl.ds(begin, GRAN)][:1])
        store_values(jnp.where(inside, v_ref[at_k], jnp.zeros((), BF)), vtx_ref, lk)
        weight = (lax.broadcasted_iota(jnp.int32, (GRAN, lk), 1) < length).astype(F32).astype(BF)
        for h in range(vtx_ref.shape[0]):
            vtx_ref[h, HD:HD + GRAN, :lk] = weight
        head_attention(keys, q_ref[at_q], vtx_ref, ctx_ref)
        c_ref[at_q] = ctx_ref[:, :lq].T

    for i in range(3):
        w_copies[i, 0].wait()

    def first(b, carry):
        project(b, h_ref[block_at(b)], 0)
        return carry
    lax.fori_loop(0, blocks, first, 0)

    for layer in range(layers):
        def attend_row(r, carry):
            @pl.when(len_ref[r] <= 128)
            def _():
                attention(r, 128, 128)

            @pl.when(len_ref[r] > 128)
            def _():
                attention(r, 256, 256)
            return carry
        lax.fori_loop(0, rows, attend_row, 0)

        for i in range(3, 6):
            w_copies[i, layer].wait()
        if layer + 1 < layers:
            for i in range(3):
                w_copies[i, layer + 1].wait()
        else:
            w_copies[6, 0].wait()
            w_copies[7, 0].wait()

        def dense(b, carry):
            at = block_at(b)
            h1 = (h_ref[at].astype(F32) + dot(c_ref[at], wo[layer])).astype(BF)
            h2 = ffn(h1, w1, w2, layer, u_ref)
            if layer + 1 < layers:
                h_ref[at] = h2
                project(b, h2, layer + 1)
            else:
                out = norm(h2)
                for i, (buf, weight, dst) in enumerate([(q_ref, cwk.at[0], ck_hbm.at[0]), (k_ref, cwv.at[0], cv_hbm.at[0]),
                                                        (v_ref, cwk.at[1], ck_hbm.at[1]), (c_ref, cwv.at[1], cv_hbm.at[1])]):
                    buf[at] = dot(out, weight[...]).astype(BF)
                    pltpu.make_async_copy(buf.at[at], dst.at[at], o_sem.at[i, b]).start()
            return carry
        lax.fori_loop(0, blocks, dense, 0)

    def finish(b, carry):
        at = block_at(b)
        for i, (buf, dst) in enumerate([(q_ref, ck_hbm.at[0]), (k_ref, cv_hbm.at[0]), (v_ref, ck_hbm.at[1]), (c_ref, cv_hbm.at[1])]):
            pltpu.make_async_copy(buf.at[at], dst.at[at], o_sem.at[i, b]).wait()
        return carry
    lax.fori_loop(0, blocks, finish, 0)


def encode(x_enc, enc_len, wq, wk, wv, wo, w1, w2, cwk, cwv):
    rows, seq, d = x_enc.shape
    layers, ff = w1.shape[0], w1.shape[2]
    heads = d // HD
    tokens = rows * seq + seq
    any_spec = pl.BlockSpec(memory_space=pl.ANY)
    big = pltpu.VMEM((tokens, d), BF)
    out = jax.ShapeDtypeStruct((layers, tokens, d), BF)
    return pl.pallas_call(
        functools.partial(encoder_kernel, rows, seq),
        out_shape=(out, out),
        in_specs=[pl.BlockSpec(memory_space=pltpu.SMEM)] + [any_spec] * 9,
        out_specs=(any_spec, any_spec),
        scratch_shapes=[big, big, big, big, big, pltpu.VMEM((BLK, ff), BF),
                        pltpu.VMEM((heads, HD + GRAN, seq), BF), pltpu.VMEM((d, seq), BF)]
        + [pltpu.VMEM(w.shape, BF) for w in (wq, wk, wv, wo, w1, w2, cwk, cwv)]
        + [pltpu.SMEM((rows,), jnp.int32), pltpu.SemaphoreType.DMA((rows,)), pltpu.SemaphoreType.DMA((layers, 8)),
           pltpu.SemaphoreType.DMA((4, tokens // BLK))],
        compiler_params=pltpu.CompilerParams(vmem_limit_bytes=60 * 1024 * 1024),
        cost_estimate=pl.CostEstimate(flops=60_000_000_000, bytes_accessed=40_000_000, transcendentals=0),
        name="encoder",
    )(enc_len, x_enc, wq, wk, wv, wo, w1, w2, cwk, cwv)


def decoder_kernel(rows, seq, per_block, len_ref, y_hbm, ck_hbm, cv_hbm, wq_h, wk_h, wv_h, wo_h, xq_h, xo_h, w1_h, w2_h, out_hbm,
                   z_ref, ck, cv, u_ref, vtx_ref, ctx_ref, cq_ref, cc_ref,
                   wq, wk, wv, wo, xq, xo, w1, w2, start_ref, y_sem, w_sem, k_sem, o_sem):
    layers = wq.shape[0]
    dec = y_hbm.shape[0] // rows
    heads = ctx_ref.shape[0] // HD
    y_copy = pltpu.make_async_copy(y_hbm, z_ref, y_sem)
    y_copy.start()
    starts = row_starts(len_ref, rows)
    for r in range(rows):
        start_ref[r] = starts[r]
    pairs = [(wq_h, wq), (wk_h, wk), (wv_h, wv), (wo_h, wo), (xq_h, xq), (xo_h, xo), (w1_h, w1), (w2_h, w2)]
    w_copies = {}

    def kv_copies(r, layer):
        at = pl.ds(pl.multiple_of(start_ref[r], GRAN), seq)
        return (pltpu.make_async_copy(ck_hbm.at[layer, at], ck.at[layer, r], k_sem.at[layer, 0, r]),
                pltpu.make_async_copy(cv_hbm.at[layer, at], cv.at[layer, r], k_sem.at[layer, 1, r]))

    for layer in range(layers):
        for i, (src, dst) in enumerate(pairs):
            w_copies[i, layer] = pltpu.make_async_copy(src.at[layer], dst.at[layer], w_sem.at[layer, i])
            if i < 6:
                w_copies[i, layer].start()
        for r in range(rows):
            for copy in kv_copies(r, layer):
                copy.start()
        for i in range(6, 8):
            w_copies[i, layer].start()
    y_copy.wait()

    m = per_block * dec
    ki = lax.broadcasted_iota(jnp.int32, (m, m), 0)
    qi = lax.broadcasted_iota(jnp.int32, (m, m), 1)
    causal = (ki <= qi) & (ki // dec == qi // dec)
    vtx_ref[:, HD:HD + GRAN, :] = jnp.ones((heads, GRAN, m), BF)
    lane = lax.broadcasted_iota(jnp.int32, (dec, heads * HD), 1)

    for layer in range(layers):
        for i in range(8):
            w_copies[i, layer].wait()

        def wait_row(r, carry):
            for copy in kv_copies(r, layer):
                copy.wait()
            return carry
        lax.fori_loop(0, rows, wait_row, 0)

        def block(b, carry):
            at = pl.ds(pl.multiple_of(b * m, m), m)
            z = z_ref[at]
            zn = norm(z)
            q = dot(zn, wq[layer]).astype(BF) * BF(HD ** -0.5)
            k = dot(zn, wk[layer]).astype(BF)
            v = dot(zn, wv[layer]).astype(BF)
            store_values(v, vtx_ref, m)
            head_attention(k, q, vtx_ref, ctx_ref, causal)
            z1 = (z.astype(F32) + dot(ctx_ref[...].T, wo[layer])).astype(BF)
            cq_ref[...] = dot(norm(z1), xq[layer]).astype(BF) * BF(HD ** -0.5)

            def cross(r, carry2):
                row = b * per_block + r
                length = len_ref[row]
                mine = pl.ds(pl.multiple_of(r * dec, dec), dec)
                qr = cq_ref[mine]
                qs = jnp.concatenate([jnp.where(lane // HD == h, qr, jnp.zeros((), BF)) for h in range(heads)], axis=0)
                s = dot_t(qs, ck[layer, row])
                s = jnp.where(lax.broadcasted_iota(jnp.int32, (1, seq), 1) < length, s, NEG)
                top = jnp.max(s, axis=1, keepdims=True)
                e = jnp.exp2((s - top) * LOG2E)
                p = (e * (1.0 / jnp.sum(e, axis=1, keepdims=True))).astype(BF)
                vals = jnp.where(lax.broadcasted_iota(jnp.int32, (seq, 1), 0) < length, cv[layer, row], jnp.zeros((), BF))
                o = dot(p, vals)
                first = lax.broadcasted_iota(jnp.int32, (dec, 2 * HD), 1) < HD
                for j in range(heads // 2):
                    cols = slice(128 * j, 128 * j + 128)
                    cc_ref[mine, cols] = jnp.where(first, o[2 * j * dec:(2 * j + 1) * dec, cols],
                                                   o[(2 * j + 1) * dec:(2 * j + 2) * dec, cols]).astype(BF)
                return carry2
            lax.fori_loop(0, per_block, cross, 0)
            z2 = (z1.astype(F32) + dot(cc_ref[...], xo[layer])).astype(BF)
            z_ref[at] = ffn(z2, w1, w2, layer, u_ref)
            return carry
        lax.fori_loop(0, rows // per_block, block, 0)

    out_copy = pltpu.make_async_copy(z_ref, out_hbm, o_sem)
    out_copy.start()
    out_copy.wait()


def decode(y, enc_len, ck, cv, seq, wq, wk, wv, wo, xq, xo, w1, w2):
    rows, dec, d = y.shape
    layers, ff = w1.shape[0], w1.shape[2]
    heads = d // HD
    per_block = BLK // dec
    any_spec = pl.BlockSpec(memory_space=pl.ANY)
    weights = (wq, wk, wv, wo, xq, xo, w1, w2)
    out = pl.pallas_call(
        functools.partial(decoder_kernel, rows, seq, per_block),
        out_shape=jax.ShapeDtypeStruct((rows * dec, d), BF),
        in_specs=[pl.BlockSpec(memory_space=pltpu.SMEM)] + [any_spec] * 11,
        out_specs=any_spec,
        scratch_shapes=[pltpu.VMEM((rows * dec, d), BF), pltpu.VMEM((layers, rows, seq, d), BF), pltpu.VMEM((layers, rows, seq, d), BF),
                        pltpu.VMEM((BLK, ff), BF), pltpu.VMEM((heads, HD + GRAN, BLK), BF), pltpu.VMEM((d, BLK), BF),
                        pltpu.VMEM((BLK, d), BF), pltpu.VMEM((BLK, d), BF)]
        + [pltpu.VMEM(w.shape, BF) for w in weights]
        + [pltpu.SMEM((rows,), jnp.int32), pltpu.SemaphoreType.DMA, pltpu.SemaphoreType.DMA((layers, 8)),
           pltpu.SemaphoreType.DMA((layers, 2, rows)), pltpu.SemaphoreType.DMA],
        compiler_params=pltpu.CompilerParams(vmem_limit_bytes=60 * 1024 * 1024),
        cost_estimate=pl.CostEstimate(flops=12_000_000_000, bytes_accessed=40_000_000, transcendentals=0),
        name="decoder",
    )(enc_len, y.reshape(rows * dec, d), ck, cv, *weights)
    return out.reshape(rows, dec, d)


def solution(mesh):
    pair_size = mesh.shape["pair"]
    to_partner = [(source, (source + pair_size // 2) % pair_size) for source in range(pair_size)]
    row_spec = P(("data", "pair"))
    full_spec = P()

    def per_device(x_enc, enc_len, y_dec, enc_wq, enc_wk, enc_wv, enc_wo, enc_w1, enc_w2, dec_wq, dec_wk, dec_wv, dec_wo, crs_wq, crs_wk, crs_wv, crs_wo, dec_w1, dec_w2):
        d = x_enc.shape[2]
        flat = lambda w: w.reshape(w.shape[0], w.shape[1] * w.shape[2], d)
        y_here = lax.ppermute(y_dec, "pair", to_partner)
        ck, cv = encode(x_enc, enc_len, enc_wq, enc_wk, enc_wv, flat(enc_wo), enc_w1, enc_w2, crs_wk, crs_wv)
        out_here = decode(y_here, enc_len, ck, cv, x_enc.shape[1], dec_wq, dec_wk, dec_wv, flat(dec_wo), crs_wq, flat(crs_wo), dec_w1, dec_w2)
        return lax.ppermute(out_here, "pair", to_partner)

    return jax.shard_map(per_device, mesh=mesh, in_specs=(row_spec, row_spec, row_spec) + (full_spec,) * 16, out_specs=row_spec, check_vma=False)
```

```python
import functools

import jax
import jax.numpy as jnp
from jax import lax
from jax.experimental import pallas as pl
from jax.experimental.pallas import tpu as pltpu
from jax.sharding import PartitionSpec as P

BF = jnp.bfloat16
F32 = jnp.float32
BLK = 256
GRAN = 16
ROWS = 2
GROUP = 2
LIMIT = 1e20
HD = 64
LOG2E = 1.4426950408889634
NEG = -1e30


def dot(a, b):
    return jnp.dot(a, b, preferred_element_type=F32)


def dot_t(a, b):
    return lax.dot_general(a, b, (((1,), (1,)), ((), ())), preferred_element_type=F32)


def norm(x):
    xw = x.astype(F32)
    return (xw * lax.rsqrt(jnp.mean(xw * xw, axis=-1, keepdims=True) + 1e-6)).astype(BF)


def gelu(x):
    inner = x * (0.7978845608028654 + 0.035677408136300125 * (x * x))
    half = 0.5 * x
    return half + half * jnp.tanh(inner)


def ffn(h1s, w1_ref, w2_ref, layer, u_ref):
    hns = [norm(h1) for h1 in h1s]
    ff = w1_ref.shape[2]
    for i, hn in enumerate(hns):
        for c in range(0, ff, 512):
            u_ref[i, :, c:c + 512] = gelu(dot(hn, w1_ref[layer, :, c:c + 512])).astype(BF)
    return [(h1.astype(F32) + dot(u_ref[i], w2_ref[layer])).astype(BF) for i, h1 in enumerate(h1s)]


def score(keys, queries, h):
    pair = slice(128 * (h // 2), 128 * (h // 2) + 128)
    lane = lax.broadcasted_iota(jnp.int32, (queries.shape[0], 2 * HD), 1)
    mine = (lane < HD) if h % 2 == 0 else (lane >= HD)
    return dot_t(keys[:, pair], jnp.where(mine, queries[:, pair], jnp.zeros((), BF)))


def weigh(s, mask=None):
    if mask is not None:
        s = jnp.where(mask, s, NEG)
    return jnp.exp2((s - jnp.max(s, axis=0, keepdims=True)) * LOG2E).astype(BF)


def head_attention(jobs, lag=2, shift=True):
    steps = [(job, h, j) for j, job in enumerate(jobs) for h in range(job[0].shape[1] // HD)]
    scores = {}
    reach = [None] * len(jobs)
    for i in range(len(steps) + lag):
        if i < len(steps):
            (keys, queries, _, _, _), h, _ = steps[i]
            scores[i] = score(keys, queries, h)
        if i >= lag:
            (keys, queries, vtx_ref, ctx_ref, mask), h, j = steps[i - lag]
            s = scores.pop(i - lag)
            e = weigh(s, mask) if shift else jnp.exp2(s * LOG2E).astype(BF)
            o = dot(vtx_ref[h, :, :keys.shape[0]], e)
            inverse = 1.0 / o[HD:HD + 1]
            ctx_ref[h * HD:(h + 1) * HD, :queries.shape[0]] = (o[:HD] * inverse).astype(BF)
            if not shift:
                far = jnp.maximum(jnp.max(jnp.abs(o[:HD + 8]), axis=0, keepdims=True), inverse)
                reach[j] = far if reach[j] is None else jnp.maximum(reach[j], far)
    return reach


def store_values(v, vtx_ref, lk):
    vt = v.T
    for h in range(v.shape[1] // HD):
        vtx_ref[h, :HD, :lk] = vt[h * HD:(h + 1) * HD]


def place_rows(len_ref, rows, start_ref, order_ref):
    lens = [len_ref[r] for r in range(rows)]
    ranks = [jnp.int32(0)] * rows
    for r in range(rows):
        for t in range(r):
            later = (lens[t] <= lens[r]).astype(jnp.int32)
            ranks[r] = ranks[r] + later
            ranks[t] = ranks[t] + 1 - later
    for r in range(rows):
        order_ref[ranks[r]] = r
    at = jnp.int32(0)
    for i in range(rows):
        r = order_ref[i]
        start_ref[r] = at
        at = at + (len_ref[r] + (GRAN - 1)) // GRAN * GRAN
    return at


def encoder_kernel(rows, seq, len_ref, x_hbm, wq_h, wk_h, wv_h, wo_h, w1_h, w2_h, cwk_h, cwv_h,
                   ck_hbm, cv_hbm,
                   h_ref, q_ref, k_ref, v_ref, c_ref, u_ref, vtx_ref, ctx_ref,
                   wq, wk, wv, wo, w1, w2, cwk, cwv, ok_ref, start_ref, order_ref, x_sem, w_sem, o_sem):
    layers = wq.shape[0]
    x_copies = [pltpu.make_async_copy(x_hbm.at[r], q_ref.at[pl.ds(r * seq, seq)], x_sem.at[r]) for r in range(rows)]
    for copy in x_copies:
        copy.start()
    pairs = [(wq_h, wq), (wk_h, wk), (wv_h, wv), (wo_h, wo), (w1_h, w1), (w2_h, w2)]
    w_copies = {}
    for layer in range(layers):
        for i, (src, dst) in enumerate(pairs):
            w_copies[i, layer] = pltpu.make_async_copy(src.at[layer], dst.at[layer], w_sem.at[layer, i])
            w_copies[i, layer].start()
    for i, (src, dst) in enumerate([(cwk_h, cwk), (cwv_h, cwv)]):
        w_copies[6 + i, 0] = pltpu.make_async_copy(src, dst, w_sem.at[0, 6 + i])
        w_copies[6 + i, 0].start()

    blocks = (place_rows(len_ref, rows, start_ref, order_ref) + (BLK - 1)) // BLK
    for copy in x_copies:
        copy.wait()

    def pack(i, carry):
        r = order_ref[i]
        h_ref[pl.ds(pl.multiple_of(start_ref[r], GRAN), seq)] = q_ref[pl.ds(pl.multiple_of(r * seq, seq), seq)]
        return carry
    lax.fori_loop(0, rows, pack, 0)

    def block_at(b):
        return pl.ds(pl.multiple_of(b * BLK, BLK), BLK)

    def project(bs, hidden, layer):
        hns = [norm(hid) for hid in hidden]
        for b, hn in zip(bs, hns):
            at = block_at(b)
            q_ref[at] = (dot(hn, wq[layer]).astype(BF) * BF(HD ** -0.5))
            k_ref[at] = dot(hn, wk[layer]).astype(BF)
            v_ref[at] = dot(hn, wv[layer]).astype(BF)

    def over_blocks(fn):
        def group(g, carry):
            fn([g * GROUP + i for i in range(GROUP)])
            return carry
        lax.fori_loop(0, blocks // GROUP, group, 0)

        @pl.when(blocks % GROUP != 0)
        def _():
            fn([blocks - 1])

    def attention(i, count, lq, lk, shift):
        jobs, dests = [], []
        for slot in range(count):
            r = order_ref[i * count + slot]
            begin = pl.multiple_of(start_ref[r], GRAN)
            length = len_ref[r]
            at_k, at_q = pl.ds(begin, lk), pl.ds(begin, lq)
            vtx, ctx = vtx_ref.at[slot], ctx_ref.at[slot]
            inside = lax.broadcasted_iota(jnp.int32, (lk, 1), 0) < length
            keys = jnp.where(inside, k_ref[at_k], k_ref[pl.ds(begin, GRAN)][:1])
            store_values(jnp.where(inside, v_ref[at_k], jnp.zeros((), BF)), vtx, lk)
            weight = (lax.broadcasted_iota(jnp.int32, (GRAN, lk), 1) < length).astype(F32).astype(BF)
            for h in range(vtx_ref.shape[1]):
                vtx[h, HD:HD + GRAN, :lk] = weight
            jobs.append((keys, q_ref[at_q], vtx, ctx, None))
            dests.append((at_q, ctx, length))
        reach = head_attention(jobs, shift=shift)
        for (at_q, ctx, length), far in zip(dests, reach):
            c_ref[at_q] = ctx[:, :lq].T
            if far is not None:
                inside = lax.broadcasted_iota(jnp.int32, (1, lq), 1) < length
                ok = jnp.where((far < LIMIT) | (~inside), 1.0, 0.0)
                ok_ref[:1, :lq] = jnp.minimum(ok_ref[:1, :lq], ok)

    for i in range(3):
        w_copies[i, 0].wait()

    over_blocks(lambda bs: project(bs, [h_ref[block_at(b)] for b in bs], 0))

    def layer_step(at_layer, carry):
        ok_ref[...] = jnp.ones(ok_ref.shape, F32)

        def attend_rows(i, carry):
            longest = len_ref[order_ref[i * ROWS + ROWS - 1]]
            for low, high in ((0, 128), (128, 192), (192, 256)):
                @pl.when((longest > low) & (longest <= high))
                def _(high=high):
                    attention(i, ROWS, (high + 127) // 128 * 128, high, False)
            return carry
        lax.fori_loop(0, rows // ROWS, attend_rows, 0)

        @pl.when(jnp.min(ok_ref[...]) < 0.5)
        def _():
            def attend_row(i, carry):
                attention(i, 1, seq, seq, True)
                return carry
            lax.fori_loop(0, rows, attend_row, 0)

        for layer in range(layers):
            @pl.when(at_layer == layer)
            def _(layer=layer):
                for i in range(3, 6):
                    w_copies[i, layer].wait()
                if layer + 1 < layers:
                    for i in range(3):
                        w_copies[i, layer + 1].wait()
                else:
                    w_copies[6, 0].wait()
                    w_copies[7, 0].wait()

                def dense(bs):
                    h1s = [(h_ref[block_at(b)].astype(F32) + dot(c_ref[block_at(b)], wo[layer])).astype(BF) for b in bs]
                    h2s = ffn(h1s, w1, w2, layer, u_ref)
                    if layer + 1 < layers:
                        for b, h2 in zip(bs, h2s):
                            h_ref[block_at(b)] = h2
                        project(bs, h2s, layer + 1)
                    else:
                        outs = [norm(h2) for h2 in h2s]
                        for b, out in zip(bs, outs):
                            at = block_at(b)
                            for i, (buf, weight, dst) in enumerate([(q_ref, cwk.at[0], ck_hbm.at[0]), (k_ref, cwv.at[0], cv_hbm.at[0]),
                                                                    (v_ref, cwk.at[1], ck_hbm.at[1]), (c_ref, cwv.at[1], cv_hbm.at[1])]):
                                buf[at] = dot(out, weight[...]).astype(BF)
                        for b in bs:
                            at = block_at(b)
                            for i, (buf, dst) in enumerate([(q_ref, ck_hbm.at[0]), (k_ref, cv_hbm.at[0]), (v_ref, ck_hbm.at[1]), (c_ref, cv_hbm.at[1])]):
                                pltpu.make_async_copy(buf.at[at], dst.at[at], o_sem.at[i, b]).start()
                over_blocks(dense)
        return carry
    lax.fori_loop(0, layers, layer_step, 0)

    def finish(b, carry):
        at = block_at(b)
        for i, (buf, dst) in enumerate([(q_ref, ck_hbm.at[0]), (k_ref, cv_hbm.at[0]), (v_ref, ck_hbm.at[1]), (c_ref, cv_hbm.at[1])]):
            pltpu.make_async_copy(buf.at[at], dst.at[at], o_sem.at[i, b]).wait()
        return carry
    lax.fori_loop(0, blocks, finish, 0)


def encode(x_enc, enc_len, wq, wk, wv, wo, w1, w2, cwk, cwv):
    rows, seq, d = x_enc.shape
    layers, ff = w1.shape[0], w1.shape[2]
    heads = d // HD
    tokens = rows * seq + seq
    any_spec = pl.BlockSpec(memory_space=pl.ANY)
    big = pltpu.VMEM((tokens, d), BF)
    out = jax.ShapeDtypeStruct((layers, tokens, d), BF)
    return pl.pallas_call(
        functools.partial(encoder_kernel, rows, seq),
        out_shape=(out, out),
        in_specs=[pl.BlockSpec(memory_space=pltpu.SMEM)] + [any_spec] * 9,
        out_specs=(any_spec, any_spec),
        scratch_shapes=[big, big, big, big, big, pltpu.VMEM((GROUP, BLK, ff), BF),
                        pltpu.VMEM((ROWS, heads, HD + GRAN, seq), BF), pltpu.VMEM((ROWS, d, seq), BF)]
        + [pltpu.VMEM(w.shape, BF) for w in (wq, wk, wv, wo, w1, w2, cwk, cwv)]
        + [pltpu.VMEM((8, seq), F32), pltpu.SMEM((rows,), jnp.int32), pltpu.SMEM((rows,), jnp.int32), pltpu.SemaphoreType.DMA((rows,)), pltpu.SemaphoreType.DMA((layers, 8)),
           pltpu.SemaphoreType.DMA((4, tokens // BLK))],
        compiler_params=pltpu.CompilerParams(vmem_limit_bytes=60 * 1024 * 1024),
        cost_estimate=pl.CostEstimate(flops=60_000_000_000, bytes_accessed=40_000_000, transcendentals=0),
        name="encoder",
    )(enc_len, x_enc, wq, wk, wv, wo, w1, w2, cwk, cwv)


def decoder_kernel(rows, seq, per_block, len_ref, y_hbm, ck_hbm, cv_hbm, wq_h, wk_h, wv_h, wo_h, xq_h, xo_h, w1_h, w2_h, out_hbm,
                   z_ref, ck, cv, u_ref, vtx_ref, ctx_ref, cq_ref, cc_ref,
                   wq, wk, wv, wo, xq, xo, w1, w2, start_ref, order_ref, y_sem, w_sem, k_sem, o_sem):
    layers = wq.shape[0]
    dec = y_hbm.shape[0] // rows
    heads = ctx_ref.shape[1] // HD
    y_copy = pltpu.make_async_copy(y_hbm, z_ref, y_sem)
    y_copy.start()
    place_rows(len_ref, rows, start_ref, order_ref)
    pairs = [(wq_h, wq), (wk_h, wk), (wv_h, wv), (wo_h, wo), (xq_h, xq), (xo_h, xo), (w1_h, w1), (w2_h, w2)]
    w_copies = {}

    def kv_copies(r, layer):
        at = pl.ds(pl.multiple_of(start_ref[r], GRAN), seq)
        return (pltpu.make_async_copy(ck_hbm.at[layer, at], ck.at[layer, r], k_sem.at[layer, 0, r]),
                pltpu.make_async_copy(cv_hbm.at[layer, at], cv.at[layer, r], k_sem.at[layer, 1, r]))

    for layer in range(layers):
        for i, (src, dst) in enumerate(pairs):
            w_copies[i, layer] = pltpu.make_async_copy(src.at[layer], dst.at[layer], w_sem.at[layer, i])
            if i < 6:
                w_copies[i, layer].start()
        for r in range(rows):
            for copy in kv_copies(r, layer):
                copy.start()
        for i in range(6, 8):
            w_copies[i, layer].start()
    y_copy.wait()

    m = per_block * dec
    ki = lax.broadcasted_iota(jnp.int32, (m, m), 0)
    qi = lax.broadcasted_iota(jnp.int32, (m, m), 1)
    causal = (ki <= qi) & (ki // dec == qi // dec)
    vtx_ref[:, :, HD:HD + GRAN, :] = jnp.ones((rows // per_block, heads, GRAN, m), BF)
    lane = lax.broadcasted_iota(jnp.int32, (dec, heads * HD), 1)

    def layer_step(layer, carry0):
        for i, (src, dst) in enumerate(pairs):
            pltpu.make_async_copy(src.at[layer], dst.at[layer], w_sem.at[layer, i]).wait()

        def wait_row(r, carry):
            for copy in kv_copies(r, layer):
                copy.wait()
            return carry
        lax.fori_loop(0, rows, wait_row, 0)

        bs = range(rows // per_block)
        z = [z_ref[b * m:(b + 1) * m] for b in bs]
        zn = [norm(x) for x in z]
        jobs = []
        for b in bs:
            q = dot(zn[b], wq[layer]).astype(BF) * BF(HD ** -0.5)
            k = dot(zn[b], wk[layer]).astype(BF)
            store_values(dot(zn[b], wv[layer]).astype(BF), vtx_ref.at[b], m)
            jobs.append((k, q, vtx_ref.at[b], ctx_ref.at[b], causal))
        head_attention(jobs)
        z1 = [(z[b].astype(F32) + dot(ctx_ref[b].T, wo[layer])).astype(BF) for b in bs]
        z1n = [norm(x) for x in z1]
        for b in bs:
            cq_ref[b * m:(b + 1) * m] = dot(z1n[b], xq[layer]).astype(BF) * BF(HD ** -0.5)

        def scores(row):
            qr = cq_ref[row * dec:(row + 1) * dec]
            qs = jnp.concatenate([jnp.where(lane // HD == h, qr, jnp.zeros((), BF)) for h in range(heads)], axis=0)
            return dot_t(qs, ck[layer, row])

        def context(row, s):
            length = len_ref[row]
            s = jnp.where(lax.broadcasted_iota(jnp.int32, (1, seq), 1) < length, s, NEG)
            top = jnp.max(s, axis=1, keepdims=True)
            e = jnp.exp2((s - top) * LOG2E)
            p = (e * (1.0 / jnp.sum(e, axis=1, keepdims=True))).astype(BF)
            vals = jnp.where(lax.broadcasted_iota(jnp.int32, (seq, 1), 0) < length, cv[layer, row], jnp.zeros((), BF))
            o = dot(p, vals)
            first = lax.broadcasted_iota(jnp.int32, (dec, 2 * HD), 1) < HD
            for j in range(heads // 2):
                cols = slice(128 * j, 128 * j + 128)
                cc_ref[row * dec:(row + 1) * dec, cols] = jnp.where(
                    first, o[2 * j * dec:(2 * j + 1) * dec, cols], o[(2 * j + 1) * dec:(2 * j + 2) * dec, cols]).astype(BF)

        pending = {}
        for i in range(rows + 2):
            if i < rows:
                pending[i] = scores(i)
            if i >= 2:
                context(i - 2, pending.pop(i - 2))
        z2 = [(z1[b].astype(F32) + dot(cc_ref[b * m:(b + 1) * m], xo[layer])).astype(BF) for b in bs]
        for b, x in zip(bs, ffn(z2, w1, w2, layer, u_ref)):
            z_ref[b * m:(b + 1) * m] = x
        return carry0
    lax.fori_loop(0, layers, layer_step, 0)

    out_copy = pltpu.make_async_copy(z_ref, out_hbm, o_sem)
    out_copy.start()
    out_copy.wait()


def decode(y, enc_len, ck, cv, seq, wq, wk, wv, wo, xq, xo, w1, w2):
    rows, dec, d = y.shape
    layers, ff = w1.shape[0], w1.shape[2]
    heads = d // HD
    per_block = BLK // dec
    groups = rows // per_block
    any_spec = pl.BlockSpec(memory_space=pl.ANY)
    weights = (wq, wk, wv, wo, xq, xo, w1, w2)
    out = pl.pallas_call(
        functools.partial(decoder_kernel, rows, seq, per_block),
        out_shape=jax.ShapeDtypeStruct((rows * dec, d), BF),
        in_specs=[pl.BlockSpec(memory_space=pltpu.SMEM)] + [any_spec] * 11,
        out_specs=any_spec,
        scratch_shapes=[pltpu.VMEM((rows * dec, d), BF), pltpu.VMEM((layers, rows, seq, d), BF), pltpu.VMEM((layers, rows, seq, d), BF),
                        pltpu.VMEM((groups, BLK, ff), BF), pltpu.VMEM((groups, heads, HD + GRAN, BLK), BF), pltpu.VMEM((groups, d, BLK), BF),
                        pltpu.VMEM((rows * dec, d), BF), pltpu.VMEM((rows * dec, d), BF)]
        + [pltpu.VMEM(w.shape, BF) for w in weights]
        + [pltpu.SMEM((rows,), jnp.int32), pltpu.SMEM((rows,), jnp.int32), pltpu.SemaphoreType.DMA, pltpu.SemaphoreType.DMA((layers, 8)),
           pltpu.SemaphoreType.DMA((layers, 2, rows)), pltpu.SemaphoreType.DMA],
        compiler_params=pltpu.CompilerParams(vmem_limit_bytes=60 * 1024 * 1024),
        cost_estimate=pl.CostEstimate(flops=12_000_000_000, bytes_accessed=40_000_000, transcendentals=0),
        name="decoder",
    )(enc_len, y.reshape(rows * dec, d), ck, cv, *weights)
    return out.reshape(rows, dec, d)


def solution(mesh):
    pair_size = mesh.shape["pair"]
    to_partner = [(source, (source + pair_size // 2) % pair_size) for source in range(pair_size)]
    row_spec = P(("data", "pair"))
    full_spec = P()

    def per_device(x_enc, enc_len, y_dec, enc_wq, enc_wk, enc_wv, enc_wo, enc_w1, enc_w2, dec_wq, dec_wk, dec_wv, dec_wo, crs_wq, crs_wk, crs_wv, crs_wo, dec_w1, dec_w2):
        d = x_enc.shape[2]
        flat = lambda w: w.reshape(w.shape[0], w.shape[1] * w.shape[2], d)
        y_here = lax.ppermute(y_dec, "pair", to_partner)
        ck, cv = encode(x_enc, enc_len, enc_wq, enc_wk, enc_wv, flat(enc_wo), enc_w1, enc_w2, crs_wk, crs_wv)
        out_here = decode(y_here, enc_len, ck, cv, x_enc.shape[1], dec_wq, dec_wk, dec_wv, flat(dec_wo), crs_wq, flat(crs_wo), dec_w1, dec_w2)
        return lax.ppermute(out_here, "pair", to_partner)

    return jax.shard_map(per_device, mesh=mesh, in_specs=(row_spec, row_spec, row_spec) + (full_spec,) * 16, out_specs=row_spec, check_vma=False)
```

```python
import functools

import jax
import jax.numpy as jnp
from jax import lax
from jax.experimental import pallas as pl
from jax.experimental.pallas import tpu as pltpu
from jax.sharding import PartitionSpec as P

BF = jnp.bfloat16
F32 = jnp.float32
BLK = 256
GRAN = 16
ROWS = 4
GROUP = 2
LAG = 5
XLAG = 3
VMEM_BYTES = 67043328
LIMIT = 1e20
HD = 64
LOG2E = 1.4426950408889634
NEG = -1e30


def dot(a, b):
    return jnp.dot(a, b, preferred_element_type=F32)


def dot_t(a, b):
    return lax.dot_general(a, b, (((1,), (1,)), ((), ())), preferred_element_type=F32)


def norm(x):
    xw = x.astype(F32)
    return (xw * lax.rsqrt(jnp.mean(xw * xw, axis=-1, keepdims=True) + 1e-6)).astype(BF)


def gelu(x):
    inner = x * (0.7978845608028654 + 0.035677408136300125 * (x * x))
    half = 0.5 * x
    return half + half * jnp.tanh(inner)


def ffn(h1s, w1_ref, w2_ref, layer, u_ref):
    hns = [norm(h1) for h1 in h1s]
    ff = w1_ref.shape[2]
    for i, hn in enumerate(hns):
        for c in range(0, ff, 512):
            u_ref[i, :, c:c + 512] = gelu(dot(hn, w1_ref[layer, :, c:c + 512])).astype(BF)
    return [(h1.astype(F32) + dot(u_ref[i], w2_ref[layer])).astype(BF) for i, h1 in enumerate(h1s)]


def score(keys, queries, h):
    pair = slice(128 * (h // 2), 128 * (h // 2) + 128)
    lane = lax.broadcasted_iota(jnp.int32, (queries.shape[0], 2 * HD), 1)
    mine = (lane < HD) if h % 2 == 0 else (lane >= HD)
    return dot_t(keys[:, pair], jnp.where(mine, queries[:, pair], jnp.zeros((), BF)))


def weigh(s, mask=None):
    if mask is not None:
        s = jnp.where(mask, s, NEG)
    return jnp.exp2((s - jnp.max(s, axis=0, keepdims=True)) * LOG2E).astype(BF)


def head_attention(jobs, lag=LAG, shift=True):
    steps = [(job, h, j) for j, job in enumerate(jobs) for h in range(job[0].shape[1] // HD)]
    scores = {}
    reach = [None] * len(jobs)
    for i in range(len(steps) + lag):
        if i < len(steps):
            (keys, queries, _, _, _), h, _ = steps[i]
            scores[i] = score(keys, queries, h)
        if i >= lag:
            (keys, queries, vtx_ref, ctx_ref, mask), h, j = steps[i - lag]
            s = scores.pop(i - lag)
            e = weigh(s, mask) if shift else jnp.exp2(s * LOG2E).astype(BF)
            o = dot(vtx_ref[h, :, :keys.shape[0]], e)
            inverse = 1.0 / o[HD:HD + 1]
            ctx_ref[h * HD:(h + 1) * HD, :queries.shape[0]] = (o[:HD] * inverse).astype(BF)
            if not shift:
                far = jnp.maximum(jnp.max(jnp.abs(o[:HD + 8]), axis=0, keepdims=True), inverse)
                reach[j] = far if reach[j] is None else jnp.maximum(reach[j], far)
    return reach


def store_values(v, vtx_ref, lk):
    vt = v.T
    for h in range(v.shape[1] // HD):
        vtx_ref[h, :HD, :lk] = vt[h * HD:(h + 1) * HD]


def place_rows(len_ref, rows, start_ref, order_ref):
    lens = [len_ref[r] for r in range(rows)]
    ranks = [jnp.int32(0)] * rows
    for r in range(rows):
        for t in range(r):
            later = (lens[t] <= lens[r]).astype(jnp.int32)
            ranks[r] = ranks[r] + later
            ranks[t] = ranks[t] + 1 - later
    for r in range(rows):
        order_ref[ranks[r]] = r
    at = jnp.int32(0)
    for i in range(rows):
        r = order_ref[i]
        start_ref[r] = at
        at = at + (len_ref[r] + (GRAN - 1)) // GRAN * GRAN
    return at


def block_at(b):
    return pl.ds(pl.multiple_of(b * BLK, BLK), BLK)


def over_blocks(blocks, fn):
    def group(g, carry):
        fn([g * GROUP + i for i in range(GROUP)])
        return carry
    lax.fori_loop(0, blocks // GROUP, group, 0)

    @pl.when(blocks % GROUP != 0)
    def _():
        fn([blocks - 1])


def project(bs, hidden, buf, wq, wk, wv):
    hns = [norm(hid) for hid in hidden]
    for b, hn in zip(bs, hns):
        at = block_at(b)
        buf[0, at] = dot(hn, wq[...]).astype(BF) * BF(HD ** -0.5)
        buf[1, at] = dot(hn, wk[...]).astype(BF)
        buf[2, at] = dot(hn, wv[...]).astype(BF)


def row_attention(len_ref, start_ref, order_ref, buf, vtx_ref, ctx_ref, ok_ref):
    rows = len_ref.shape[0]
    seq = vtx_ref.shape[3]

    def attention(i, count, lq, lk, shift):
        jobs, dests = [], []
        for slot in range(count):
            r = order_ref[i * count + slot]
            begin = pl.multiple_of(start_ref[r], GRAN)
            length = len_ref[r]
            at_k, at_q = pl.ds(begin, lk), pl.ds(begin, lq)
            vtx, ctx = vtx_ref.at[slot], ctx_ref.at[slot]
            inside = lax.broadcasted_iota(jnp.int32, (lk, 1), 0) < length
            keys = jnp.where(inside, buf[1, at_k], buf[1, pl.ds(begin, GRAN)][:1])
            store_values(jnp.where(inside, buf[2, at_k], jnp.zeros((), BF)), vtx, lk)
            weight = (lax.broadcasted_iota(jnp.int32, (GRAN, lk), 1) < length).astype(F32).astype(BF)
            for h in range(vtx_ref.shape[1]):
                vtx[h, HD:HD + GRAN, :lk] = weight
            jobs.append((keys, buf[0, at_q], vtx, ctx, None))
            dests.append((at_q, ctx, length))
        reach = head_attention(jobs, shift=shift)
        for (at_q, ctx, length), far in zip(dests, reach):
            buf[3, at_q] = ctx[:, :lq].T
            if far is not None:
                inside = lax.broadcasted_iota(jnp.int32, (1, lq), 1) < length
                ok = jnp.where((far < LIMIT) | (~inside), 1.0, 0.0)
                ok_ref[:1, :lq] = jnp.minimum(ok_ref[:1, :lq], ok)

    ok_ref[...] = jnp.ones(ok_ref.shape, F32)

    def attend_rows(i, carry):
        longest = len_ref[order_ref[i * ROWS + ROWS - 1]]
        for low, high in ((0, 128), (128, 192), (192, 256)):
            @pl.when((longest > low) & (longest <= high))
            def _(high=high):
                attention(i, ROWS, (high + 127) // 128 * 128, high, False)
        return carry
    lax.fori_loop(0, rows // ROWS, attend_rows, 0)

    @pl.when(jnp.min(ok_ref[...]) < 0.5)
    def _():
        def attend_row(i, carry):
            attention(i, 1, seq, seq, True)
            return carry
        lax.fori_loop(0, rows, attend_row, 0)


def front_kernel(rows, seq, len_ref, x_hbm, wq_h, wk_h, wv_h, h_hbm, c_hbm,
                 h_ref, buf, vtx_ref, ctx_ref, wq, wk, wv, ok_ref, start_ref, order_ref, x_sem, w_sem, o_sem):
    def x_copy(r):
        return pltpu.make_async_copy(x_hbm.at[r], buf.at[3, pl.ds(pl.multiple_of(r * seq, seq), seq)], x_sem.at[r])

    for r in range(rows):
        x_copy(r).start()
    w_copies = [pltpu.make_async_copy(src.at[0], dst, w_sem.at[i]) for i, (src, dst) in enumerate([(wq_h, wq), (wk_h, wk), (wv_h, wv)])]
    for copy in w_copies:
        copy.start()
    blocks = (place_rows(len_ref, rows, start_ref, order_ref) + (BLK - 1)) // BLK

    def pack(i, carry):
        r = order_ref[i]
        x_copy(r).wait()
        h_ref[pl.ds(pl.multiple_of(start_ref[r], GRAN), seq)] = buf[3, pl.ds(pl.multiple_of(r * seq, seq), seq)]
        return carry
    lax.fori_loop(0, rows, pack, 0)
    for copy in w_copies:
        copy.wait()

    def h_copy(b):
        return pltpu.make_async_copy(h_ref.at[block_at(b)], h_hbm.at[block_at(b)], o_sem.at[0, b])

    def c_copy(b):
        return pltpu.make_async_copy(buf.at[3, block_at(b)], c_hbm.at[block_at(b)], o_sem.at[1, b])

    def first(bs):
        for b in bs:
            h_copy(b).start()
        project(bs, [h_ref[block_at(b)] for b in bs], buf, wq, wk, wv)
    over_blocks(blocks, first)
    row_attention(len_ref, start_ref, order_ref, buf, vtx_ref, ctx_ref, ok_ref)

    def send(b, carry):
        c_copy(b).start()
        return carry
    lax.fori_loop(0, blocks, send, 0)

    def finish(b, carry):
        h_copy(b).wait()
        c_copy(b).wait()
        return carry
    lax.fori_loop(0, blocks, finish, 0)


def front(x_enc, enc_len, wq, wk, wv):
    rows, seq, d = x_enc.shape
    heads = d // HD
    tokens = rows * seq + seq
    any_spec = pl.BlockSpec(memory_space=pl.ANY)
    out = jax.ShapeDtypeStruct((tokens, d), BF)
    return pl.pallas_call(
        functools.partial(front_kernel, rows, seq),
        out_shape=(out, out),
        in_specs=[pl.BlockSpec(memory_space=pltpu.SMEM)] + [any_spec] * 4,
        out_specs=(any_spec, any_spec),
        scratch_shapes=[pltpu.VMEM((tokens, d), BF), pltpu.VMEM((4, tokens, d), BF),
                        pltpu.VMEM((ROWS, heads, HD + GRAN, seq), BF), pltpu.VMEM((ROWS, d, seq), BF)]
        + [pltpu.VMEM(w.shape[1:], BF) for w in (wq, wk, wv)]
        + [pltpu.VMEM((8, seq), F32), pltpu.SMEM((rows,), jnp.int32), pltpu.SMEM((rows,), jnp.int32),
           pltpu.SemaphoreType.DMA((rows,)), pltpu.SemaphoreType.DMA((3,)), pltpu.SemaphoreType.DMA((2, tokens // BLK))],
        compiler_params=pltpu.CompilerParams(vmem_limit_bytes=50 * 1024 * 1024),
        cost_estimate=pl.CostEstimate(flops=30_000_000_000, bytes_accessed=15_000_000, transcendentals=0),
        name="front",
    )(enc_len, x_enc, wq, wk, wv)


def back_kernel(rows, seq, len_ref, h_hbm, c_hbm, y_hbm, wq_h, wk_h, wv_h, wo_h, w1_h, w2_h, cwk_h, cwv_h,
                dq_h, dk_h, dv_h, do_h, xq_h, xo_h, d1_h, d2_h, out_hbm,
                h_ref, buf, u_ref, vtx_ref, ctx_ref, z_ref, cq_ref, cc_ref,
                wq, wk, wv, wo, w1, w2, cwk, cwv, dq, dk, dv, do, xq, xo, d1, d2,
                ok_ref, start_ref, order_ref, t_sem, e_sem, d_sem, y_sem):
    layers = wo_h.shape[0]
    blocks = (place_rows(len_ref, rows, start_ref, order_ref) + (BLK - 1)) // BLK

    def token_copies(b):
        at = block_at(b)
        return (pltpu.make_async_copy(h_hbm.at[at], h_ref.at[at], t_sem.at[0, b]),
                pltpu.make_async_copy(c_hbm.at[at], buf.at[3, at], t_sem.at[1, b]))

    def start_tokens(b, carry):
        for copy in token_copies(b):
            copy.start()
        return carry

    enc = [(wo_h, wo), (w1_h, w1), (w2_h, w2), (cwk_h, cwk), (cwv_h, cwv)]
    qkv = [(wq_h, wq), (wk_h, wk), (wv_h, wv)]
    dec_pairs = [(dq_h, dq), (dk_h, dk), (dv_h, dv), (do_h, do), (xq_h, xq), (xo_h, xo), (d1_h, d1), (d2_h, d2)]

    def enc_copy(i, layer):
        return pltpu.make_async_copy(enc[i][0].at[layer], enc[i][1].at[layer], e_sem.at[i, layer])

    def qkv_copy(i, layer):
        return pltpu.make_async_copy(qkv[i][0].at[layer], qkv[i][1].at[layer - 1], e_sem.at[5 + i, layer])

    def dec_copy(i, layer):
        return pltpu.make_async_copy(dec_pairs[i][0].at[layer], dec_pairs[i][1].at[layer], d_sem.at[i, layer])

    enc_copy(0, 0).start()
    lax.fori_loop(0, jnp.minimum(blocks, GROUP), start_tokens, 0)
    enc_copy(1, 0).start()
    enc_copy(2, 0).start()
    for layer in range(1, layers):
        for i in range(3):
            qkv_copy(i, layer).start()
    lax.fori_loop(GROUP, blocks, start_tokens, 0)
    for layer in range(1, layers):
        for i in range(3):
            enc_copy(i, layer).start()
    for layer in range(layers):
        for i in range(3, 5):
            enc_copy(i, layer).start()
    y_copy = pltpu.make_async_copy(y_hbm, z_ref, y_sem)
    y_copy.start()
    for layer in range(layers):
        for i in range(8):
            dec_copy(i, layer).start()

    for layer in range(layers):
        if layer > 0:
            row_attention(len_ref, start_ref, order_ref, buf, vtx_ref, ctx_ref, ok_ref)
        for i in range(3):
            enc_copy(i, layer).wait()
        if layer + 1 < layers:
            for i in range(3):
                qkv_copy(i, layer + 1).wait()
        else:
            for other in range(layers):
                for i in range(3, 5):
                    enc_copy(i, other).wait()

        def dense(bs, layer=layer):
            if layer == 0:
                for b in bs:
                    for copy in token_copies(b):
                        copy.wait()
            h1s = [(h_ref[block_at(b)].astype(F32) + dot(buf[3, block_at(b)], wo[layer])).astype(BF) for b in bs]
            h2s = ffn(h1s, w1, w2, layer, u_ref)
            if layer + 1 < layers:
                for b, h2 in zip(bs, h2s):
                    h_ref[block_at(b)] = h2
                project(bs, h2s, buf, wq.at[layer], wk.at[layer], wv.at[layer])
            else:
                outs = [norm(h2) for h2 in h2s]
                for b, out in zip(bs, outs):
                    for other in range(layers):
                        buf[2 * other, block_at(b)] = dot(out, cwk[other]).astype(BF)
                        buf[2 * other + 1, block_at(b)] = dot(out, cwv[other]).astype(BF)
        over_blocks(blocks, dense)

    dec = y_hbm.shape[0] // rows
    m = BLK
    per_block = m // dec
    heads = ctx_ref.shape[1] // HD
    bs = range(rows // per_block)
    y_copy.wait()
    ki = lax.broadcasted_iota(jnp.int32, (m, m), 0)
    qi = lax.broadcasted_iota(jnp.int32, (m, m), 1)
    causal = (ki <= qi) & (ki // dec == qi // dec)
    for b in bs:
        vtx_ref[b, :, HD:HD + GRAN, :] = jnp.ones((heads, GRAN, m), BF)
    lane = lax.broadcasted_iota(jnp.int32, (dec, heads * HD), 1)

    def layer_step(layer, carry):
        for i in range(8):
            dec_copy(i, layer).wait()
        z = [z_ref[b * m:(b + 1) * m] for b in bs]
        zn = [norm(x) for x in z]
        jobs = []
        for b in bs:
            q = dot(zn[b], dq[layer]).astype(BF) * BF(HD ** -0.5)
            k = dot(zn[b], dk[layer]).astype(BF)
            store_values(dot(zn[b], dv[layer]).astype(BF), vtx_ref.at[b], m)
            jobs.append((k, q, vtx_ref.at[b], ctx_ref.at[b], causal))
        head_attention(jobs)
        z1 = [(z[b].astype(F32) + dot(ctx_ref[b].T, do[layer])).astype(BF) for b in bs]
        z1n = [norm(x) for x in z1]
        for b in bs:
            cq_ref[b * m:(b + 1) * m] = dot(z1n[b], xq[layer]).astype(BF) * BF(HD ** -0.5)

        def scores(row):
            qr = cq_ref[row * dec:(row + 1) * dec]
            qs = jnp.concatenate([jnp.where(lane // HD == h, qr, jnp.zeros((), BF)) for h in range(heads)], axis=0)
            return dot_t(qs, buf[2 * layer, pl.ds(pl.multiple_of(start_ref[row], GRAN), seq)])

        def context(row, s):
            length = len_ref[row]
            s = jnp.where(lax.broadcasted_iota(jnp.int32, (1, seq), 1) < length, s, NEG)
            top = jnp.max(s, axis=1, keepdims=True)
            e = jnp.exp2((s - top) * LOG2E)
            p = (e * (1.0 / jnp.sum(e, axis=1, keepdims=True))).astype(BF)
            vals = buf[2 * layer + 1, pl.ds(pl.multiple_of(start_ref[row], GRAN), seq)]
            vals = jnp.where(lax.broadcasted_iota(jnp.int32, (seq, 1), 0) < length, vals, jnp.zeros((), BF))
            o = dot(p, vals)
            first = lax.broadcasted_iota(jnp.int32, (dec, 2 * HD), 1) < HD
            for j in range(heads // 2):
                cols = slice(128 * j, 128 * j + 128)
                cc_ref[row * dec:(row + 1) * dec, cols] = jnp.where(
                    first, o[2 * j * dec:(2 * j + 1) * dec, cols], o[(2 * j + 1) * dec:(2 * j + 2) * dec, cols]).astype(BF)

        pending = {}
        for i in range(rows + XLAG):
            if i < rows:
                pending[i] = scores(i)
            if i >= XLAG:
                context(i - XLAG, pending.pop(i - XLAG))
        z2 = [(z1[b].astype(F32) + dot(cc_ref[b * m:(b + 1) * m], xo[layer])).astype(BF) for b in bs]
        for b, x in zip(bs, ffn(z2, d1, d2, layer, u_ref)):
            z_ref[b * m:(b + 1) * m] = x
        return carry
    lax.fori_loop(0, layers, layer_step, 0)

    out_copy = pltpu.make_async_copy(z_ref, out_hbm, y_sem)
    out_copy.start()
    out_copy.wait()


def back(enc_len, h, c, y, seq, enc_weights, dec_weights):
    rows, dec, d = y.shape
    wq, wk, wv, wo, w1, w2, cwk, cwv = enc_weights
    layers, ff = w1.shape[0], w1.shape[2]
    heads = d // HD
    tokens = h.shape[0]
    any_spec = pl.BlockSpec(memory_space=pl.ANY)
    out = pl.pallas_call(
        functools.partial(back_kernel, rows, seq),
        out_shape=jax.ShapeDtypeStruct((rows * dec, d), BF),
        in_specs=[pl.BlockSpec(memory_space=pltpu.SMEM)] + [any_spec] * 19,
        out_specs=any_spec,
        scratch_shapes=[pltpu.VMEM((tokens, d), BF), pltpu.VMEM((4, tokens, d), BF), pltpu.VMEM((GROUP, BLK, ff), BF),
                        pltpu.VMEM((ROWS, heads, HD + GRAN, seq), BF), pltpu.VMEM((ROWS, d, seq), BF),
                        pltpu.VMEM((rows * dec, d), BF), pltpu.VMEM((rows * dec, d), BF), pltpu.VMEM((rows * dec, d), BF)]
        + [pltpu.VMEM((layers - 1,) + w.shape[1:], BF) for w in (wq, wk, wv)]
        + [pltpu.VMEM(w.shape, BF) for w in (wo, w1, w2, cwk, cwv) + dec_weights]
        + [pltpu.VMEM((8, seq), F32), pltpu.SMEM((rows,), jnp.int32), pltpu.SMEM((rows,), jnp.int32),
           pltpu.SemaphoreType.DMA((2, tokens // BLK)), pltpu.SemaphoreType.DMA((8, layers)), pltpu.SemaphoreType.DMA((8, layers)), pltpu.SemaphoreType.DMA],
        compiler_params=pltpu.CompilerParams(vmem_limit_bytes=VMEM_BYTES),
        cost_estimate=pl.CostEstimate(flops=60_000_000_000, bytes_accessed=40_000_000, transcendentals=0),
        name="back",
    )(enc_len, h, c, y.reshape(rows * dec, d), *enc_weights, *dec_weights)
    return out.reshape(rows, dec, d)


def solution(mesh):
    pair_size = mesh.shape["pair"]
    to_partner = [(source, (source + pair_size // 2) % pair_size) for source in range(pair_size)]
    row_spec = P(("data", "pair"))
    full_spec = P()

    def per_device(x_enc, enc_len, y_dec, enc_wq, enc_wk, enc_wv, enc_wo, enc_w1, enc_w2, dec_wq, dec_wk, dec_wv, dec_wo, crs_wq, crs_wk, crs_wv, crs_wo, dec_w1, dec_w2):
        d = x_enc.shape[2]
        flat = lambda w: w.reshape(w.shape[0], w.shape[1] * w.shape[2], d)
        y_here = lax.ppermute(y_dec, "pair", to_partner)
        h, c = front(x_enc, enc_len, enc_wq, enc_wk, enc_wv)
        out_here = back(enc_len, h, c, y_here, x_enc.shape[1],
                        (enc_wq, enc_wk, enc_wv, flat(enc_wo), enc_w1, enc_w2, crs_wk, crs_wv),
                        (dec_wq, dec_wk, dec_wv, flat(dec_wo), crs_wq, flat(crs_wo), dec_w1, dec_w2))
        return lax.ppermute(out_here, "pair", to_partner)

    return jax.shard_map(per_device, mesh=mesh, in_specs=(row_spec, row_spec, row_spec) + (full_spec,) * 16, out_specs=row_spec, check_vma=False)
```

```python
import functools

import jax
import jax.numpy as jnp
from jax import lax
from jax.experimental import pallas as pl
from jax.experimental.pallas import tpu as pltpu
from jax.sharding import PartitionSpec as P

BF = jnp.bfloat16
F32 = jnp.float32
BLK = 256
GRAN = 16
ROWS = 4
GROUP = 2
LAG = 5
XLAG = 3
VMEM_BYTES = 67043328
LIMIT = 1e20
HD = 64
LOG2E = 1.4426950408889634
NEG = -1e30


def dot(a, b):
    return jnp.dot(a, b, preferred_element_type=F32)


def dot_t(a, b):
    return lax.dot_general(a, b, (((1,), (1,)), ((), ())), preferred_element_type=F32)


def norm(x, scale=1.0):
    xw = x.astype(F32)
    inv_rms = lax.rsqrt(jnp.mean(xw * xw, axis=-1, keepdims=True) + 1e-6)
    return (xw * (inv_rms * scale)).astype(BF)


def gelu_of_half(half):
    inner = half * (2 * 0.7978845608028654 + 8 * 0.035677408136300125 * (half * half))
    return half + half * jnp.tanh(inner)


def ffn(h1s, w1_ref, w2_ref, layer, u_ref):
    hns = [norm(h1, 0.5) for h1 in h1s]
    ff = w1_ref.shape[2]
    for i, hn in enumerate(hns):
        for c in range(0, ff, 512):
            u_ref[i, :, c:c + 512] = gelu_of_half(dot(hn, w1_ref[layer, :, c:c + 512])).astype(BF)
    return [(h1.astype(F32) + dot(u_ref[i], w2_ref[layer])).astype(BF) for i, h1 in enumerate(h1s)]


def score(keys, queries, h):
    pair = slice(128 * (h // 2), 128 * (h // 2) + 128)
    lane = lax.broadcasted_iota(jnp.int32, (keys.shape[0], 2 * HD), 1)
    mine = (lane < HD) if h % 2 == 0 else (lane >= HD)
    return dot_t(jnp.where(mine, keys[:, pair], jnp.zeros((), BF)), queries[:, pair])


def weigh(s, mask=None):
    if mask is not None:
        s = jnp.where(mask, s, NEG)
    return jnp.exp2((s - jnp.max(s, axis=0, keepdims=True)) * LOG2E).astype(BF)


def head_attention(jobs, lag=LAG, shift=True):
    steps = [(job, h, j) for j, job in enumerate(jobs) for h in range(job[0].shape[1] // HD)]
    scores = {}
    reach = [None] * len(jobs)
    for i in range(len(steps) + lag):
        if i < len(steps):
            (keys, queries, _, _, _), h, _ = steps[i]
            scores[i] = score(keys, queries, h)
        if i >= lag:
            (keys, queries, vtx_ref, ctx_ref, mask), h, j = steps[i - lag]
            s = scores.pop(i - lag)
            e = weigh(s, mask) if shift else jnp.exp2(s * LOG2E).astype(BF)
            o = dot(vtx_ref[h, :, :keys.shape[0]], e)
            inverse = 1.0 / o[HD:HD + 1]
            ctx_ref[h * HD:(h + 1) * HD, :queries.shape[0]] = (o[:HD] * inverse).astype(BF)
            if not shift:
                far = jnp.maximum(jnp.max(jnp.abs(o[:HD + 8]), axis=0, keepdims=True), inverse)
                reach[j] = far if reach[j] is None else jnp.maximum(reach[j], far)
    return reach


def store_values(v, vtx_ref, lk):
    vt = v.T
    for h in range(v.shape[1] // HD):
        vtx_ref[h, :HD, :lk] = vt[h * HD:(h + 1) * HD]


def place_rows(len_ref, rows, start_ref, order_ref):
    lens = [len_ref[r] for r in range(rows)]
    ranks = [jnp.int32(0)] * rows
    for r in range(rows):
        for t in range(r):
            later = (lens[t] <= lens[r]).astype(jnp.int32)
            ranks[r] = ranks[r] + later
            ranks[t] = ranks[t] + 1 - later
    for r in range(rows):
        order_ref[ranks[r]] = r
    at = jnp.int32(0)
    for i in range(rows):
        r = order_ref[i]
        start_ref[r] = at
        at = at + (len_ref[r] + (GRAN - 1)) // GRAN * GRAN
    return at


def block_at(b):
    return pl.ds(pl.multiple_of(b * BLK, BLK), BLK)


def over_blocks(blocks, fn):
    def group(g, carry):
        fn([g * GROUP + i for i in range(GROUP)])
        return carry
    lax.fori_loop(0, blocks // GROUP, group, 0)

    @pl.when(blocks % GROUP != 0)
    def _():
        fn([blocks - 1])


def project(bs, hidden, buf, wq, wk, wv):
    hns = [norm(hid) for hid in hidden]
    for b, hn in zip(bs, hns):
        at = block_at(b)
        buf[0, at] = dot(hn, wq[...]).astype(BF) * BF(HD ** -0.5)
        buf[1, at] = dot(hn, wk[...]).astype(BF)
        buf[2, at] = dot(hn, wv[...]).astype(BF)


def row_attention(len_ref, start_ref, order_ref, buf, vtx_ref, ctx_ref, ok_ref):
    rows = len_ref.shape[0]
    seq = vtx_ref.shape[3]

    def attention(i, count, lq, lk, shift):
        jobs, dests = [], []
        for slot in range(count):
            r = order_ref[i * count + slot]
            begin = pl.multiple_of(start_ref[r], GRAN)
            length = len_ref[r]
            at_k, at_q = pl.ds(begin, lk), pl.ds(begin, lq)
            vtx, ctx = vtx_ref.at[slot], ctx_ref.at[slot]
            inside = lax.broadcasted_iota(jnp.int32, (lk, 1), 0) < length
            keys = jnp.where(inside, buf[1, at_k], buf[1, pl.ds(begin, GRAN)][:1])
            store_values(jnp.where(inside, buf[2, at_k], jnp.zeros((), BF)), vtx, lk)
            weight = (lax.broadcasted_iota(jnp.int32, (GRAN, lk), 1) < length).astype(F32).astype(BF)
            for h in range(vtx_ref.shape[1]):
                vtx[h, HD:HD + GRAN, :lk] = weight
            jobs.append((keys, buf[0, at_q], vtx, ctx, None))
            dests.append((at_q, ctx, length))
        reach = head_attention(jobs, shift=shift)
        for (at_q, ctx, length), far in zip(dests, reach):
            buf[3, at_q] = ctx[:, :lq].T
            if far is not None:
                inside = lax.broadcasted_iota(jnp.int32, (1, lq), 1) < length
                ok = jnp.where((far < LIMIT) | (~inside), 1.0, 0.0)
                ok_ref[:1, :lq] = jnp.minimum(ok_ref[:1, :lq], ok)

    ok_ref[...] = jnp.ones(ok_ref.shape, F32)

    def attend_rows(i, carry):
        longest = len_ref[order_ref[i * ROWS + ROWS - 1]]
        for low, high in ((0, 128), (128, 192), (192, 256)):
            @pl.when((longest > low) & (longest <= high))
            def _(high=high):
                attention(i, ROWS, (high + 127) // 128 * 128, high, False)
        return carry
    lax.fori_loop(0, rows // ROWS, attend_rows, 0)

    @pl.when(jnp.min(ok_ref[...]) < 0.5)
    def _():
        def attend_row(i, carry):
            attention(i, 1, seq, seq, True)
            return carry
        lax.fori_loop(0, rows, attend_row, 0)


def front_kernel(rows, seq, len_ref, x_hbm, wq_h, wk_h, wv_h, h_hbm, c_hbm,
                 h_ref, buf, vtx_ref, ctx_ref, wq, wk, wv, ok_ref, start_ref, order_ref, x_sem, w_sem, o_sem):
    def x_copy(r):
        return pltpu.make_async_copy(x_hbm.at[r], buf.at[3, pl.ds(pl.multiple_of(r * seq, seq), seq)], x_sem.at[r])

    for r in range(rows):
        x_copy(r).start()
    w_copies = [pltpu.make_async_copy(src.at[0], dst, w_sem.at[i]) for i, (src, dst) in enumerate([(wq_h, wq), (wk_h, wk), (wv_h, wv)])]
    for copy in w_copies:
        copy.start()
    blocks = (place_rows(len_ref, rows, start_ref, order_ref) + (BLK - 1)) // BLK

    def pack(i, carry):
        r = order_ref[i]
        x_copy(r).wait()
        h_ref[pl.ds(pl.multiple_of(start_ref[r], GRAN), seq)] = buf[3, pl.ds(pl.multiple_of(r * seq, seq), seq)]
        return carry
    lax.fori_loop(0, rows, pack, 0)
    for copy in w_copies:
        copy.wait()

    def h_copy(b):
        return pltpu.make_async_copy(h_ref.at[block_at(b)], h_hbm.at[block_at(b)], o_sem.at[0, b])

    def c_copy(b):
        return pltpu.make_async_copy(buf.at[3, block_at(b)], c_hbm.at[block_at(b)], o_sem.at[1, b])

    def first(bs):
        for b in bs:
            h_copy(b).start()
        project(bs, [h_ref[block_at(b)] for b in bs], buf, wq, wk, wv)
    over_blocks(blocks, first)
    row_attention(len_ref, start_ref, order_ref, buf, vtx_ref, ctx_ref, ok_ref)

    def send(b, carry):
        c_copy(b).start()
        return carry
    lax.fori_loop(0, blocks, send, 0)

    def finish(b, carry):
        h_copy(b).wait()
        c_copy(b).wait()
        return carry
    lax.fori_loop(0, blocks, finish, 0)


def front(x_enc, enc_len, wq, wk, wv):
    rows, seq, d = x_enc.shape
    heads = d // HD
    tokens = rows * seq + seq
    any_spec = pl.BlockSpec(memory_space=pl.ANY)
    out = jax.ShapeDtypeStruct((tokens, d), BF)
    return pl.pallas_call(
        functools.partial(front_kernel, rows, seq),
        out_shape=(out, out),
        in_specs=[pl.BlockSpec(memory_space=pltpu.SMEM)] + [any_spec] * 4,
        out_specs=(any_spec, any_spec),
        scratch_shapes=[pltpu.VMEM((tokens, d), BF), pltpu.VMEM((4, tokens, d), BF),
                        pltpu.VMEM((ROWS, heads, HD + GRAN, seq), BF), pltpu.VMEM((ROWS, d, seq), BF)]
        + [pltpu.VMEM(w.shape[1:], BF) for w in (wq, wk, wv)]
        + [pltpu.VMEM((8, seq), F32), pltpu.SMEM((rows,), jnp.int32), pltpu.SMEM((rows,), jnp.int32),
           pltpu.SemaphoreType.DMA((rows,)), pltpu.SemaphoreType.DMA((3,)), pltpu.SemaphoreType.DMA((2, tokens // BLK))],
        compiler_params=pltpu.CompilerParams(vmem_limit_bytes=VMEM_BYTES),
        cost_estimate=pl.CostEstimate(flops=30_000_000_000, bytes_accessed=15_000_000, transcendentals=0),
        name="front",
    )(enc_len, x_enc, wq, wk, wv)


def back_kernel(rows, seq, len_ref, h_hbm, c_hbm, y_hbm, wq_h, wk_h, wv_h, wo_h, w1_h, w2_h, cwk_h, cwv_h,
                dq_h, dk_h, dv_h, do_h, xq_h, xo_h, d1_h, d2_h, out_hbm,
                h_ref, buf, u_ref, vtx_ref, ctx_ref, z_ref, cq_ref, cc_ref,
                wq, wk, wv, wo, w1, w2, cwk, cwv, dq, dk, dv, do, xq, xo, d1, d2,
                ok_ref, start_ref, order_ref, t_sem, e_sem, d_sem, y_sem):
    layers = wo_h.shape[0]
    blocks = (place_rows(len_ref, rows, start_ref, order_ref) + (BLK - 1)) // BLK

    def token_copies(b):
        at = block_at(b)
        return (pltpu.make_async_copy(h_hbm.at[at], h_ref.at[at], t_sem.at[0, b]),
                pltpu.make_async_copy(c_hbm.at[at], buf.at[3, at], t_sem.at[1, b]))

    def start_tokens(b, carry):
        for copy in token_copies(b):
            copy.start()
        return carry

    enc = [(wo_h, wo), (w1_h, w1), (w2_h, w2), (cwk_h, cwk), (cwv_h, cwv)]
    qkv = [(wq_h, wq), (wk_h, wk), (wv_h, wv)]
    dec_pairs = [(dq_h, dq), (dk_h, dk), (dv_h, dv), (do_h, do), (xq_h, xq), (xo_h, xo), (d1_h, d1), (d2_h, d2)]

    def enc_copy(i, layer):
        return pltpu.make_async_copy(enc[i][0].at[layer], enc[i][1].at[layer], e_sem.at[i, layer])

    def qkv_copy(i, layer):
        return pltpu.make_async_copy(qkv[i][0].at[layer], qkv[i][1].at[layer - 1], e_sem.at[5 + i, layer])

    def dec_copy(i, layer):
        return pltpu.make_async_copy(dec_pairs[i][0].at[layer], dec_pairs[i][1].at[layer], d_sem.at[i, layer])

    enc_copy(0, 0).start()
    lax.fori_loop(0, jnp.minimum(blocks, GROUP), start_tokens, 0)
    enc_copy(1, 0).start()
    enc_copy(2, 0).start()
    for layer in range(1, layers):
        for i in range(3):
            qkv_copy(i, layer).start()
    lax.fori_loop(GROUP, blocks, start_tokens, 0)
    for layer in range(1, layers):
        for i in range(3):
            enc_copy(i, layer).start()
    for layer in range(layers):
        for i in range(3, 5):
            enc_copy(i, layer).start()
    y_copy = pltpu.make_async_copy(y_hbm, z_ref, y_sem)
    y_copy.start()
    for layer in range(layers):
        for i in range(8):
            dec_copy(i, layer).start()

    for layer in range(layers):
        if layer > 0:
            row_attention(len_ref, start_ref, order_ref, buf, vtx_ref, ctx_ref, ok_ref)
        for i in range(3):
            enc_copy(i, layer).wait()
        if layer + 1 < layers:
            for i in range(3):
                qkv_copy(i, layer + 1).wait()
        else:
            for other in range(layers):
                for i in range(3, 5):
                    enc_copy(i, other).wait()

        def dense(bs, layer=layer):
            if layer == 0:
                for b in bs:
                    for copy in token_copies(b):
                        copy.wait()
            h1s = [(h_ref[block_at(b)].astype(F32) + dot(buf[3, block_at(b)], wo[layer])).astype(BF) for b in bs]
            h2s = ffn(h1s, w1, w2, layer, u_ref)
            if layer + 1 < layers:
                for b, h2 in zip(bs, h2s):
                    h_ref[block_at(b)] = h2
                project(bs, h2s, buf, wq.at[layer], wk.at[layer], wv.at[layer])
            else:
                outs = [norm(h2) for h2 in h2s]
                for b, out in zip(bs, outs):
                    for other in range(layers):
                        buf[2 * other, block_at(b)] = dot(out, cwk[other]).astype(BF)
                        buf[2 * other + 1, block_at(b)] = dot(out, cwv[other]).astype(BF)
        over_blocks(blocks, dense)

    dec = y_hbm.shape[0] // rows
    m = BLK
    per_block = m // dec
    heads = ctx_ref.shape[1] // HD
    bs = range(rows // per_block)
    y_copy.wait()
    ki = lax.broadcasted_iota(jnp.int32, (m, m), 0)
    qi = lax.broadcasted_iota(jnp.int32, (m, m), 1)
    causal = (ki <= qi) & (ki // dec == qi // dec)
    for b in bs:
        vtx_ref[b, :, HD:HD + GRAN, :] = jnp.ones((heads, GRAN, m), BF)

    def layer_step(layer, carry):
        for i in range(8):
            dec_copy(i, layer).wait()
        z = [z_ref[b * m:(b + 1) * m] for b in bs]
        zn = [norm(x) for x in z]
        jobs = []
        for b in bs:
            q = dot(zn[b], dq[layer]).astype(BF) * BF(HD ** -0.5)
            k = dot(zn[b], dk[layer]).astype(BF)
            store_values(dot(zn[b], dv[layer]).astype(BF), vtx_ref.at[b], m)
            jobs.append((k, q, vtx_ref.at[b], ctx_ref.at[b], causal))
        head_attention(jobs)
        z1 = [(z[b].astype(F32) + dot(ctx_ref[b].T, do[layer])).astype(BF) for b in bs]
        z1n = [norm(x) for x in z1]
        for b in bs:
            cq_ref[b * m:(b + 1) * m] = dot(z1n[b], xq[layer]).astype(BF) * BF(HD ** -0.5)

        def scores(row):
            qr = cq_ref[row * dec:(row + 1) * dec]
            keys = buf[2 * layer, pl.ds(pl.multiple_of(start_ref[row], GRAN), seq)]
            first = lax.broadcasted_iota(jnp.int32, (dec, 2 * HD), 1) < HD
            parts = []
            for j in range(heads // 2):
                cols = slice(128 * j, 128 * j + 128)
                zero = jnp.zeros((), BF)
                qs = jnp.concatenate([jnp.where(first, qr[:, cols], zero), jnp.where(first, zero, qr[:, cols])], axis=0)
                parts.append(dot_t(qs, keys[:, cols]))
            return jnp.concatenate(parts, axis=0)

        def context(row, s):
            length = len_ref[row]
            s = jnp.where(lax.broadcasted_iota(jnp.int32, (1, seq), 1) < length, s, NEG)
            top = jnp.max(s, axis=1, keepdims=True)
            e = jnp.exp2((s - top) * LOG2E)
            p = (e * (1.0 / jnp.sum(e, axis=1, keepdims=True))).astype(BF)
            vals = buf[2 * layer + 1, pl.ds(pl.multiple_of(start_ref[row], GRAN), seq)]
            vals = jnp.where(lax.broadcasted_iota(jnp.int32, (seq, 1), 0) < length, vals, jnp.zeros((), BF))
            o = dot(p, vals)
            first = lax.broadcasted_iota(jnp.int32, (dec, 2 * HD), 1) < HD
            for j in range(heads // 2):
                cols = slice(128 * j, 128 * j + 128)
                cc_ref[row * dec:(row + 1) * dec, cols] = jnp.where(
                    first, o[2 * j * dec:(2 * j + 1) * dec, cols], o[(2 * j + 1) * dec:(2 * j + 2) * dec, cols]).astype(BF)

        pending = {}
        for i in range(rows + XLAG):
            if i < rows:
                pending[i] = scores(i)
            if i >= XLAG:
                context(i - XLAG, pending.pop(i - XLAG))
        z2 = [(z1[b].astype(F32) + dot(cc_ref[b * m:(b + 1) * m], xo[layer])).astype(BF) for b in bs]
        for b, x in zip(bs, ffn(z2, d1, d2, layer, u_ref)):
            z_ref[b * m:(b + 1) * m] = x
        return carry
    lax.fori_loop(0, layers, layer_step, 0)

    out_copy = pltpu.make_async_copy(z_ref, out_hbm, y_sem)
    out_copy.start()
    out_copy.wait()


def back(enc_len, h, c, y, seq, enc_weights, dec_weights):
    rows, dec, d = y.shape
    wq, wk, wv, wo, w1, w2, cwk, cwv = enc_weights
    layers, ff = w1.shape[0], w1.shape[2]
    heads = d // HD
    tokens = h.shape[0]
    any_spec = pl.BlockSpec(memory_space=pl.ANY)
    out = pl.pallas_call(
        functools.partial(back_kernel, rows, seq),
        out_shape=jax.ShapeDtypeStruct((rows * dec, d), BF),
        in_specs=[pl.BlockSpec(memory_space=pltpu.SMEM)] + [any_spec] * 19,
        out_specs=any_spec,
        scratch_shapes=[pltpu.VMEM((tokens, d), BF), pltpu.VMEM((4, tokens, d), BF), pltpu.VMEM((GROUP, BLK, ff), BF),
                        pltpu.VMEM((ROWS, heads, HD + GRAN, seq), BF), pltpu.VMEM((ROWS, d, seq), BF),
                        pltpu.VMEM((rows * dec, d), BF), pltpu.VMEM((rows * dec, d), BF), pltpu.VMEM((rows * dec, d), BF)]
        + [pltpu.VMEM((layers - 1,) + w.shape[1:], BF) for w in (wq, wk, wv)]
        + [pltpu.VMEM(w.shape, BF) for w in (wo, w1, w2, cwk, cwv) + dec_weights]
        + [pltpu.VMEM((8, seq), F32), pltpu.SMEM((rows,), jnp.int32), pltpu.SMEM((rows,), jnp.int32),
           pltpu.SemaphoreType.DMA((2, tokens // BLK)), pltpu.SemaphoreType.DMA((8, layers)), pltpu.SemaphoreType.DMA((8, layers)), pltpu.SemaphoreType.DMA],
        compiler_params=pltpu.CompilerParams(vmem_limit_bytes=VMEM_BYTES),
        cost_estimate=pl.CostEstimate(flops=60_000_000_000, bytes_accessed=40_000_000, transcendentals=0),
        name="back",
    )(enc_len, h, c, y.reshape(rows * dec, d), *enc_weights, *dec_weights)
    return out.reshape(rows, dec, d)


def solution(mesh):
    pair_size = mesh.shape["pair"]
    to_partner = [(source, (source + pair_size // 2) % pair_size) for source in range(pair_size)]
    row_spec = P(("data", "pair"))
    full_spec = P()

    def per_device(x_enc, enc_len, y_dec, enc_wq, enc_wk, enc_wv, enc_wo, enc_w1, enc_w2, dec_wq, dec_wk, dec_wv, dec_wo, crs_wq, crs_wk, crs_wv, crs_wo, dec_w1, dec_w2):
        d = x_enc.shape[2]
        flat = lambda w: w.reshape(w.shape[0], w.shape[1] * w.shape[2], d)
        y_here = lax.ppermute(y_dec, "pair", to_partner)
        h, c = front(x_enc, enc_len, enc_wq, enc_wk, enc_wv)
        out_here = back(enc_len, h, c, y_here, x_enc.shape[1],
                        (enc_wq, enc_wk, enc_wv, flat(enc_wo), enc_w1, enc_w2, crs_wk, crs_wv),
                        (dec_wq, dec_wk, dec_wv, flat(dec_wo), crs_wq, flat(crs_wo), dec_w1, dec_w2))
        return lax.ppermute(out_here, "pair", to_partner)

    return jax.shard_map(per_device, mesh=mesh, in_specs=(row_spec, row_spec, row_spec) + (full_spec,) * 16, out_specs=row_spec, check_vma=False)
```
